512 devices in a mesh: tm: 128 (over x, z, core), space: 4 (over y).
Axes of the slice: x: 4, y: 4, z: 16, core: 2. Of those that a mesh axis runs over, the one named last changes fastest.
Arguments:
- forcing: bfloat16 [2048, 256, 256], P('tm', 'space'), may hold values from -0.59765625 to 0.59765625
- starting_heat: bfloat16 [256, 256], P('space'), may hold values from -3 to 3, as said below
Outputs:
- heat_history: float32 [2048, 256, 256], P('tm', 'space')
- history: float32 [2, 512], P(None, 'tm')
- change: float32 [2, 512], P(None, 'tm')
The draws below stay inside these ranges and needn't reach their ends.
Inputs may be any that keep to these rules, and one draw needn't show every extreme that they name: starting_heat is a combination of the 64 sine modes with both indices from 1 to 8, scaled so that its largest magnitude is 3.
All inputs are finite; a program needn't handle non-finite values.
Results may differ from the reference program's by a relative error of at most 0.0016.
Values may be sent and summed in bfloat16 or wider, within the bound.
A program may use at most 64 MiB of HBM per device.

```python
import math
import jax
import jax.numpy as jnp
from jax import lax

GRID = 256
FINE_FACTOR = 4
COARSE_FACTOR = 4
ITERS = 2
NT = 2048
C_POINTS = 512
TOP_POINTS = 128


def draw_starting_heat(key, part):
    mode_index = jnp.arange(1, 9, dtype=jnp.int32)
    cell_index = jnp.arange(1, GRID + 1, dtype=jnp.int32)
    product = mode_index[:, None] * cell_index[None, :] % (2 * (GRID + 1))
    sine_rows = jnp.sin(jnp.pi * product.astype(jnp.float32) / (GRID + 1))
    weights = jax.random.normal(key, (8, 8), jnp.float32)
    inner = jnp.dot(weights, sine_rows, precision=lax.Precision.HIGHEST)
    summed = jnp.dot(sine_rows.T, inner, precision=lax.Precision.HIGHEST)
    scaled = 3.0 * summed / jnp.max(jnp.abs(summed))
    return scaled.astype(jnp.bfloat16)


def block_scale(rng, dims, cuts, low, top_value):
    gain = 1.0
    for axis_at, parts in cuts:
        draws = jax.random.uniform(jax.random.fold_in(jax.random.fold_in(rng, 6), axis_at), (parts,), jnp.float32, low / len(cuts), top_value / len(cuts))
        gain = gain * jnp.repeat(jnp.exp(draws), dims[axis_at] // parts).reshape((-1,) + (1,) * (len(dims) - 1 - axis_at))
    return gain


def bell_draw(stream_key, extent, spread, reach, shards=(), kind=jnp.bfloat16):
    level = block_scale(stream_key, extent, shards, -0.22, 0.18) if shards else 1.0
    result = jax.random.normal(stream_key, extent, jnp.float32) * spread * level
    return jnp.minimum(jnp.maximum(result, -reach), reach).astype(kind)


def setup_inputs(seed: int = 0) -> dict:
    keys = jax.random.split(jax.random.key(seed), 3)
    forcing = bell_draw(keys[0], (NT, GRID, GRID), 0.1, 0.59765625, ((0, 128), (1, 4)))
    starting_heat = draw_starting_heat(jax.random.fold_in(keys[2], 71), 0)
    return dict(forcing=forcing, starting_heat=starting_heat)


DURATION = 0.004

def sine_table(sample_locations, number_type):
    numbers = jnp.arange(1, sample_locations + 1, dtype=jnp.int32)
    product = numbers[:, None] * numbers[None, :] % (2 * (sample_locations + 1))
    angles = jnp.pi * product.astype(jnp.float32) / (sample_locations + 1)
    return (math.sqrt(2.0 / (sample_locations + 1)) * jnp.sin(angles)).astype(number_type)

def eigenvalues(sample_locations, first_mode, mode_count):
    numbers = (first_mode + jnp.arange(mode_count, dtype=jnp.int32) + 1).astype(jnp.float32)
    halves = jnp.sin(jnp.pi * numbers / (2 * (sample_locations + 1)))
    return 4.0 * (sample_locations + 1) ** 2 * halves * halves

def smoothing_pass(starts, sources, factor):
    current = starts
    visited = []
    for column in range(sources.shape[1] - 1):
        current = factor * current + sources[:, column]
        visited.append(current)
    return visited

def forward_block(field_block, table_half):
    halved = jnp.dot(field_block.reshape(-1, GRID), table_half, preferred_element_type=jnp.float32)
    halved = lax.optimization_barrier(halved.astype(jnp.bfloat16).reshape(field_block.shape))
    return jnp.einsum('xi,tiy->txy', table_half.astype(jnp.float32), halved.astype(jnp.float32), precision=lax.Precision.HIGHEST)

def reference(forcing, starting_heat):
    table_half = sine_table(GRID, jnp.bfloat16)
    table_full = sine_table(GRID, jnp.float32)
    decay_rates = eigenvalues(GRID, 0, GRID)[:, None] + eigenvalues(GRID, 0, GRID)[None, :]
    increment_duration = DURATION / NT
    per_increment_factor = 1.0 / (1.0 + increment_duration * decay_rates)
    mid_gain = 1.0 / (1.0 + FINE_FACTOR * increment_duration * decay_rates)
    top_gain = 1.0 / (1.0 + FINE_FACTOR * COARSE_FACTOR * increment_duration * decay_rates)
    start_field = forward_block(starting_heat[None], table_half)[0]

    def source_block(field_block):
        return per_increment_factor * forward_block(field_block, table_half)
    grouped = forcing.reshape(C_POINTS, FINE_FACTOR, GRID, GRID)
    sources = lax.map(source_block, grouped)
    values = jnp.zeros((C_POINTS, GRID, GRID), jnp.float32)
    history_rows = []
    change_rows = []
    for iteration in range(ITERS):
        begins = jnp.concatenate([start_field[None], values[:-1]], 0)
        ends_one = smoothing_pass(begins, sources, per_increment_factor)[-1]
        relaxed = per_increment_factor * ends_one + sources[:, -1]
        ends_two = smoothing_pass(jnp.concatenate([start_field[None], relaxed[:-1]], 0), sources, per_increment_factor)[-1]
        residual = sources[:, -1] + per_increment_factor * ends_two - relaxed
        history_rows.append(jnp.sqrt(lax.optimization_barrier(jnp.sum(residual * residual, axis=(1, 2))) / (GRID * GRID)))
        coarse_rhs = residual.reshape(TOP_POINTS, COARSE_FACTOR, GRID, GRID)
        running = coarse_rhs[:, 0]
        for column in range(1, COARSE_FACTOR):
            running = mid_gain * running + coarse_rhs[:, column]

        def advance(carried, source):
            updated = top_gain * carried + source
            return (updated, updated)
        unused, coarse_values = lax.scan(advance, jnp.zeros((GRID, GRID), jnp.float32), running)
        begins = jnp.concatenate([jnp.zeros((1, GRID, GRID), jnp.float32), coarse_values[:-1]], 0)
        pieces = smoothing_pass(begins, coarse_rhs, mid_gain)
        correction = jnp.stack(pieces + [coarse_values], axis=1).reshape(C_POINTS, GRID, GRID)
        values = relaxed + correction
        corr_sq = lax.optimization_barrier(jnp.sum(correction * correction, axis=(1, 2)))
        value_sq = lax.optimization_barrier(jnp.sum(values * values, axis=(1, 2)))
        change_rows.append(jnp.sqrt(corr_sq / value_sq))
    starts = jnp.concatenate([start_field[None], values[:-1]], 0)

    def finish(items):
        begin_value, block_sources, end_value = items
        inside = smoothing_pass(begin_value[None], block_sources[None], per_increment_factor)
        spectral_path = jnp.concatenate([jnp.stack(inside, axis=1)[0], end_value[None]], 0)
        rows_back = jnp.einsum('xi,tiy->txy', table_full, spectral_path, precision=lax.Precision.HIGHEST)
        rows_back = lax.optimization_barrier(rows_back.astype(jnp.bfloat16))
        return jnp.einsum('txi,iy->txy', rows_back.astype(jnp.float32), table_half.astype(jnp.float32), precision=lax.Precision.HIGHEST)
    heat_history = lax.map(finish, (starts, sources, values)).reshape(NT, GRID, GRID)
    return (heat_history, jnp.stack(history_rows), jnp.stack(change_rows))
```

```python
import math

import jax
import jax.numpy as jnp
import numpy as np
from jax import lax
from jax.experimental import pallas as pl
from jax.experimental.pallas import tpu as pltpu
from jax.sharding import Mesh
from jax.sharding import PartitionSpec as P

GRID = 256
NT = 2048
STEP = 0.004 / NT
X, Z, CORE, Y = "tm_0", "tm_1", "tm_2", "space"
NX, NZ = 4, 16
PHASES = 4
F32, BF16 = jnp.float32, jnp.bfloat16


def sine_tables():
    numbers = np.arange(1, GRID + 1)
    product = numbers[:, None] * numbers[None, :] % (2 * (GRID + 1))
    angles = (np.float32(np.pi) * product.astype(np.float32)) / np.float32(GRID + 1)
    table = (np.float32(math.sqrt(2.0 / (GRID + 1))) * np.sin(angles.astype(np.float64))).astype(np.float32)
    half = table.astype(jnp.bfloat16)
    rest = (table - half.astype(np.float32)).astype(jnp.bfloat16)
    return half, rest


def mode_tables():
    mu = (4.0 * (GRID + 1) ** 2 * np.sin(np.pi * np.arange(1, GRID + 1) / (2 * (GRID + 1))) ** 2).astype(np.float32)
    lane = np.arange(128)
    rows = np.broadcast_to(mu[:, None], (GRID, 128))
    packed = mu[64 * (lane // 32)[None, :] + np.arange(64)[:, None]]
    tiles = np.concatenate([packed.reshape(NZ, 4, 128)] * 2, axis=1)
    columns = np.broadcast_to(mu.reshape(8, 1, 32)[:, :, lane % 32], (8, 8, 128))
    return tuple(np.ascontiguousarray(t) for t in (rows, packed, tiles, columns))


def lane_group():
    return lax.broadcasted_iota(jnp.int32, (64, 128), 1) // 32


def turn(parts):
    group = lane_group()
    rolled = [parts[0]] + [pltpu.roll(parts[a], 32 * a, 1) for a in range(1, 4)]
    out = []
    for b in range(4):
        pick = [rolled[(g - b) % 4] for g in range(4)]
        mixed = jnp.where(
            group < 2, jnp.where(group == 0, pick[0], pick[1]), jnp.where(group == 2, pick[2], pick[3])
        )
        out.append(pltpu.roll(mixed, 128 - 32 * b, 1) if b else mixed)
    return out


def dot(a, b):
    return jnp.dot(a, b, preferred_element_type=F32)


class Weights:
    def __init__(self, x):
        one = 1.0
        gain = one / (one + x)
        y = 4.0 * x
        psi = one / (one + y)
        self.lift = lift = one + 16.0 * x
        theta = one / lift
        square = gain * gain
        phi = square * square
        psi2 = psi * psi
        psi3 = psi2 * psi
        psi4 = psi2 * psi2
        less = -(x * x * (6.0 + 4.0 * x + x * x)) * phi * psi
        deep = -(y * y * (6.0 + 4.0 * y + y * y)) * psi4 * theta
        big = phi * less
        alpha = 3.0 * big * psi2
        beta = psi3 * (big * psi3 + phi * deep)
        xb = psi3 * phi * lift
        c2 = psi4 * psi * big * phi - beta * xb
        c1 = 2.0 * big * phi * psi - alpha * xb
        kappa = (less * psi3 + deep) * lift
        bl2 = beta * lift * lift
        w1 = (phi * psi2, phi * psi, phi, xb)
        own = (psi4 * big * phi * lift, psi3 * big * phi * lift, None, (c1 + c2 * lift) * lift)
        w3 = tuple(bl2 * a if b is None else bl2 * a - b for a, b in zip(w1, own))
        self.w1 = w1
        self.w2 = (big * phi - w3[0], -w3[1], -w3[2], -w3[3])
        self.w3 = w3
        self.w4 = (less * phi * psi - kappa * w1[0], less * phi - kappa * w1[1], -kappa * w1[2], -kappa * w1[3])
        self.d2 = less * phi * psi2 - kappa * psi3 * phi
        self.e2 = -c2 * lift
        self.alpha = alpha + beta * lift
        self.gain, self.phi, self.psi, self.theta = gain, phi, psi, theta
        self.less, self.deep, self.xb, self.kappa = less, deep, xb, kappa


def weighted(weights, parts):
    total = weights[0] * parts[0]
    for w, part in zip(weights[1:], parts[1:]):
        total = total + w * part
    return total


def corrections(w, first, residual):
    out = []
    p, q = first, None
    for c in range(3):
        p = w.psi * p + residual[c]
        q = residual[c] if q is None else w.psi * q + residual[c]
        out.append(p)
    out.append(w.theta * first + (w.psi * q + residual[3]))
    return out


def kernel(
    forcing, starting, sine, sine_rest, mu_rows, mu_packed, mu_tiles, mu_columns,
    heat, history, change,
    fin, sin, sh, sr, mrow, mpack, mtile, mcol,
    send_a, recv_a, send_u, recv_u, start_c, src, send_n, recv_n,
    send_z, recv_z, send_x, recv_x, send_b, recv_b, send_o, recv_o, send_s, recv_s, hout,
    load_sem, store_sem, sa, ra, su, ru, sn, rn, sz, rz, sx, rx, sb, rb, so, ro, ss, rs,
):
    x, z, core, y = (lax.axis_index(a) for a in (X, Z, CORE, Y))
    me = 2 * y + core
    zn, zp = lax.rem(z + 1, NZ), lax.rem(z + NZ - 1, NZ)
    xn = jnp.where(z == NZ - 1, lax.rem(x + 1, NX), x)
    xp = jnp.where(z == 0, lax.rem(x + NX - 1, NX), x)
    my_rows = pl.ds(pl.multiple_of(64 * y, 64), 64)

    loads = [
        (forcing, fin), (sine, sh), (sine_rest, sr), (starting, sin), (mu_rows, mrow), (mu_packed, mpack),
        (mu_tiles.at[z], mtile), (mu_columns.at[me], mcol),
    ]
    loads = [pltpu.make_async_copy(a, b, load_sem.at[i]) for i, (a, b) in enumerate(loads)]
    for copy in loads:
        copy.start()

    barrier = pltpu.get_barrier_semaphore()
    for k in range(1, 8):
        d = lax.rem(me + k, 8)
        pl.semaphore_signal(barrier, inc=1, device_id={Y: d // 2, CORE: lax.rem(d, 2)})
    for k in range(1, NZ):
        pl.semaphore_signal(barrier, inc=1, device_id={Z: lax.rem(z + k, NZ)})
    for k in range(1, NX):
        pl.semaphore_signal(barrier, inc=1, device_id={X: lax.rem(x + k, NX)})
    pl.semaphore_signal(barrier, inc=1, device_id={X: xn, Z: zn})
    pl.semaphore_signal(barrier, inc=1, device_id={X: xp, Z: zp})

    loads[0].wait()
    loads[1].wait()
    table = sh[...]

    def halves(p):
        fields = jnp.concatenate([fin[4 * c + p] for c in range(4)], axis=0)
        product = dot(fields, table)
        for side in range(2):
            for q, part in enumerate(turn([product[64 * c : 64 * c + 64, 128 * side : 128 * side + 128] for c in range(4)])):
                send_a[p, 4 * side + q] = part.astype(BF16)

    def copy_a(p, d, source, from_core, rows):
        return pltpu.make_async_remote_copy(
            src_ref=send_a.at[p, d], dst_ref=recv_a.at[p, from_core, rows],
            send_sem=sa.at[p, d], recv_sem=ra.at[p, source], device_id={Y: d // 2, CORE: d % 2},
        )

    for p in range(PHASES):
        halves(p)
        if p == 0:
            pl.semaphore_wait(barrier, 27)
        for d in range(8):
            @pl.when(d != me)
            def _():
                copy_a(p, d, me, core, my_rows).start()

            @pl.when(d == me)
            def _():
                recv_a[p, core, my_rows] = send_a[p, d]

    first = jnp.logical_and(x == 0, z == 0)
    loads[3].wait()

    def copy_u(k, source):
        return pltpu.make_async_remote_copy(
            src_ref=send_u.at[k], dst_ref=recv_u.at[pl.ds(pl.multiple_of(64 * source, 64), 64)],
            send_sem=su.at[k], recv_sem=ru.at[source], device_id={Y: k},
        )

    @pl.when(first)
    def _():
        product = dot(sin[...], table)
        for k in range(4):
            side = product[:, 128 * (k // 2) : 128 * (k // 2) + 128]
            shift = 2 * (k % 2)
            even = pltpu.roll(side, (128 - 32 * shift) % 128, 1) if shift else side
            odd = pltpu.roll(side, (128 - 32 * (shift + 1)) % 128, 1)
            send_u[k] = jnp.where(core == 0, even, odd).astype(BF16)
        for k in range(4):
            @pl.when(k != y)
            def _():
                copy_u(k, y).start()

            @pl.when(k == y)
            def _():
                recv_u[my_rows] = send_u[k]

    for i in (2, 4, 5, 6, 7):
        loads[i].wait()
    gain = 1.0 / (1.0 + STEP * (mrow[...] + mcol[0:1, :]))
    w = Weights(STEP * (mpack[...] + mcol[0:1, :]))
    wo = Weights(STEP * (mtile[...] + mcol[...]))
    lower = lax.broadcasted_iota(jnp.int32, (8, 128), 0) < 4
    hop = wo.theta * wo.theta
    cross = jnp.where(lower, 0.0, 2.0 * wo.theta * wo.alpha)
    powers = [(jnp.ones_like(hop), jnp.zeros_like(hop))]
    for k in range(NZ):
        t, c = powers[-1]
        powers.append((hop * t, hop * c + cross * t))

    @pl.when(first)
    def _():
        for k in range(4):
            @pl.when(k != y)
            def _():
                copy_u(k, k).wait_recv()
        modes = dot(table, recv_u[...])
        group = lane_group()
        total = jnp.where(group == 0, modes[0:64], 0.0)
        for r in range(1, 4):
            total = jnp.where(group == r, pltpu.roll(modes[64 * r : 64 * r + 64], 32 * r, 1), total)
        start_c[...] = total

    @pl.when(jnp.logical_not(first))
    def _():
        start_c[...] = jnp.zeros_like(start_c)

    for p in range(PHASES):
        for s in range(8):
            @pl.when(s != me)
            def _():
                copy_a(p, s, s, s % 2, pl.ds(64 * (s // 2), 64)).wait_recv()
        for h in range(2):
            src[p, h] = gain * dot(table, recv_a[p, h])

    points = []
    for h in range(2):
        s = gain * src[0, h] + src[1, h]
        s = gain * s + src[2, h]
        s = gain * s + src[3, h]
        points.append(turn([s[64 * r : 64 * r + 64] for r in range(4)]))
    start = start_c[...]
    points[0][0] = points[0][0] + w.phi * start

    f = [weighted(w.w1, points[h]) for h in range(2)]
    g = [weighted(w.w2, points[h]) for h in range(2)]
    f_all = w.theta * f[0] + f[1]
    g_all = w.theta * g[0] + w.alpha * f[0] + g[1]
    for v in range(8):
        a, b = f_all[8 * v : 8 * v + 8], g_all[8 * v : 8 * v + 8]
        send_z[2 * v] = jnp.where(lower, a, pltpu.roll(b, 4, 0))
        send_z[2 * v + 1] = jnp.where(lower, pltpu.roll(a, 4, 0), b)

    def copy_z(to, source):
        return pltpu.make_async_remote_copy(
            src_ref=send_z.at[to], dst_ref=recv_z.at[source],
            send_sem=sz.at[to], recv_sem=rz.at[source], device_id={Z: to},
        )

    far_first = sorted(range(1, NZ), key=lambda k: -min(k, NZ - k))
    for k in far_first:
        copy_z(lax.rem(z + k, NZ), z).start()
    recv_z[z] = send_z[z]

    send_n[0] = points[1][3]
    send_n[1] = weighted(w.w4, points[1]) + w.d2 * points[0][3]
    send_n[2] = weighted(w.w3, points[1]) + w.e2 * points[0][3]
    copy_n = pltpu.make_async_remote_copy(
        src_ref=send_n, dst_ref=recv_n, send_sem=sn, recv_sem=rn, device_id={X: xn, Z: zn}
    )
    copy_n.start()

    for k in far_first[::-1]:
        source = lax.rem(z + k, NZ)
        copy_z(source, source).wait_recv()
    plain, coupled = [jnp.zeros((8, 128), F32)], [jnp.zeros((8, 128), F32)]
    for k in range(NZ):
        plain.append(hop * plain[-1] + recv_z[k])
    for k in range(NZ):
        coupled.append(hop * coupled[-1] + cross * pltpu.roll(plain[k], 4, 0))
    states = [a + b for a, b in zip(plain, coupled)]
    send_x[...] = states[NZ]

    def copy_x(to, source, k):
        return pltpu.make_async_remote_copy(
            src_ref=send_x, dst_ref=recv_x.at[source], send_sem=sx.at[k], recv_sem=rx.at[source], device_id={X: to}
        )

    for k in range(1, NX):
        copy_x(lax.rem(x + k, NX), x, k).start()
    for k in range(1, NX):
        source = lax.rem(x + k, NX)
        copy_x(source, source, k).wait_recv()
    recv_x[x] = states[NZ]
    entering = jnp.zeros((8, 128), F32)
    for k in range(NX - 1):
        further = powers[NZ][0] * entering + powers[NZ][1] * pltpu.roll(entering, 4, 0) + recv_x[k]
        entering = jnp.where(k < x, further, entering)
    turned = pltpu.roll(entering, 4, 0)
    for k in range(NZ):
        send_b[k] = states[k] + (powers[k][0] * entering + powers[k][1] * turned)

    def copy_b(to, source):
        return pltpu.make_async_remote_copy(
            src_ref=send_b.at[to], dst_ref=recv_b.at[source],
            send_sem=sb.at[to], recv_sem=rb.at[source], device_id={Z: to},
        )

    for k in far_first:
        copy_b(lax.rem(z + k, NZ), z).start()
    recv_b[z] = send_b[z]

    copy_n.wait_recv()
    keep = jnp.logical_not(first)
    near = [jnp.where(keep, recv_n[i], 0.0) for i in range(3)]
    residual_a = [near[0], points[0][3]]
    near_d = [near[1], weighted(w.w4, points[0]) + w.d2 * near[0]]
    near_e = [near[2], weighted(w.w3, points[0]) + w.e2 * near[0]]

    for k in far_first[::-1]:
        source = lax.rem(z + k, NZ)
        copy_b(source, source).wait_recv()
    fs, gs = [], []
    for v in range(8):
        a, b = recv_b[2 * v], recv_b[2 * v + 1]
        fs.append(jnp.where(lower, a, pltpu.roll(b, 4, 0)))
        gs.append(jnp.where(lower, pltpu.roll(a, 4, 0), b))
    f_in = jnp.concatenate(fs, axis=0)
    g_in = jnp.concatenate(gs, axis=0)

    sums = []
    for h in range(2):
        if h == 1:
            g_in = w.theta * g_in + w.alpha * f_in + g[0]
            f_in = w.theta * f_in + f[0]
        s = points[h]
        a = residual_a[h]
        e1 = f_in - w.xb * a
        d = w.kappa * f_in + near_d[h]
        e2 = g_in + near_e[h]
        r1 = [w.phi * a] + [w.phi * s[c] for c in range(3)]
        p1 = corrections(w, e1, r1)
        later = [w.less * e1, w.less * p1[0], w.less * p1[1], w.less * p1[2] + w.deep * e1]
        r2 = [w.phi * d] + [w.phi * later[c] for c in range(3)]
        p2 = corrections(w, e2, r2)
        v1 = [s[c] + p1[c] for c in range(4)]
        v2 = [v1[c] + later[c] + p2[c] for c in range(4)]
        enter = a + e1 + d + e2
        if h == 0:
            enter = enter + start
        squares = [jnp.sum(q * q, axis=0, keepdims=True) for q in r1 + r2 + p1 + p2 + v1 + v2]
        sums.append(squares)
        begin = jnp.concatenate(turn([enter, v2[0], v2[1], v2[2]]), axis=0)
        ends = jnp.concatenate(turn(v2), axis=0)
        u = begin
        for p in range(3):
            u = gain * u + src[p, h]
            src[p, h] = u
        src[3, h] = ends

    def copy_o(p, h, k, source):
        return pltpu.make_async_remote_copy(
            src_ref=send_o.at[p, h, pl.ds(64 * k, 64)], dst_ref=recv_o.at[p, source],
            send_sem=so.at[p, h, k], recv_sem=ro.at[p, source], device_id={Y: k, CORE: h},
        )

    rest = sr[...]
    for p in range(PHASES):
        for h in range(2):
            u = src[p, h]
            high = u.astype(BF16)
            low = (u - high.astype(F32)).astype(BF16)
            send_o[p, h] = (dot(table, high) + (dot(table, low) + dot(rest, high))).astype(BF16)
        for h in range(2):
            for k in range(4):
                @pl.when(2 * k + h != me)
                def _():
                    copy_o(p, h, k, me).start()

                @pl.when(2 * k + h == me)
                def _():
                    recv_o[p, me] = send_o[p, h, 64 * k : 64 * k + 64]

    def copy_s(h, k, source):
        return pltpu.make_async_remote_copy(
            src_ref=send_s.at[h], dst_ref=recv_s.at[source],
            send_sem=ss.at[h, k], recv_sem=rs.at[source], device_id={Y: k, CORE: h},
        )

    for h in range(2):
        send_s[h] = jnp.concatenate(sums[h], axis=0)
    for h in range(2):
        for k in range(4):
            @pl.when(2 * k + h != me)
            def _():
                copy_s(h, k, me).start()

            @pl.when(2 * k + h == me)
            def _():
                recv_s[me] = send_s[h]

    stores = []
    for p in range(PHASES):
        for s in range(8):
            @pl.when(s != me)
            def _():
                copy_o(p, s % 2, s // 2, s).wait_recv()
        sides = []
        for side in range(2):
            sides.append(turn([recv_o[p, 4 * side + q].astype(F32) for q in range(4)]))
        rows = jnp.concatenate(
            [jnp.concatenate([sides[0][c], sides[1][c]], axis=1) for c in range(4)], axis=0
        ).astype(BF16)
        field = dot(rows, table)
        for c in range(4):
            hout[4 * c + p] = field[64 * c : 64 * c + 64]
            stores.append(pltpu.make_async_copy(hout.at[4 * c + p], heat.at[4 * c + p], store_sem.at[4 * c + p]))
            stores[-1].start()

    for s in range(8):
        @pl.when(s != me)
        def _():
            copy_s(s % 2, s // 2, s).wait_recv()
    total = recv_s[0]
    for s in range(1, 8):
        total = total + recv_s[s]
    total = jnp.sum(total, axis=1, keepdims=True)
    norms = jnp.sqrt(total[0:8] / (GRID * GRID))
    ratios = jnp.sqrt(total[8:16] / total[16:24])
    mine = lax.broadcasted_iota(jnp.int32, (8, 128), 1) == lax.broadcasted_iota(jnp.int32, (8, 128), 0) % 4
    for column, out in ((norms, history), (ratios, change)):
        spread = jnp.where(mine, column, 0.0)
        for i in range(2):
            out[i : i + 1, :] = jnp.sum(spread[4 * i : 4 * i + 4], axis=0, keepdims=True)[:, 0:4]

    for p in range(PHASES):
        for d in range(8):
            @pl.when(d != me)
            def _():
                copy_a(p, d, me, core, my_rows).wait_send()
                copy_o(p, d % 2, d // 2, me).wait_send()

    for d in range(8):
        @pl.when(d != me)
        def _():
            copy_s(d % 2, d // 2, me).wait_send()

    @pl.when(first)
    def _():
        for k in range(4):
            @pl.when(k != y)
            def _():
                copy_u(k, y).wait_send()

    copy_n.wait_send()
    for k in range(1, NZ):
        to = lax.rem(z + k, NZ)
        copy_z(to, z).wait_send()
        copy_b(to, z).wait_send()
    for k in range(1, NX):
        copy_x(lax.rem(x + k, NX), x, k).wait_send()
    for copy in stores:
        copy.wait()


def per_device(forcing, starting_heat):
    half, rest = sine_tables()
    tables = mode_tables()
    anywhere = pl.BlockSpec(memory_space=pl.ANY)
    vmem = pl.BlockSpec(memory_space=pltpu.VMEM)
    dma = pltpu.SemaphoreType.DMA
    scratch = [
        pltpu.VMEM((16, 64, 256), BF16), pltpu.VMEM((64, 256), BF16),
        pltpu.VMEM((256, 256), BF16), pltpu.VMEM((256, 256), BF16),
        pltpu.VMEM((256, 128), F32), pltpu.VMEM((64, 128), F32),
        pltpu.VMEM((8, 128), F32), pltpu.VMEM((8, 128), F32),
        pltpu.VMEM((4, 8, 64, 128), BF16), pltpu.VMEM((4, 2, 256, 128), BF16),
        pltpu.VMEM((4, 64, 128), BF16), pltpu.VMEM((256, 128), BF16), pltpu.VMEM((64, 128), F32),
        pltpu.VMEM((4, 2, 256, 128), F32), pltpu.VMEM((3, 64, 128), F32), pltpu.VMEM((3, 64, 128), F32),
        pltpu.VMEM((16, 8, 128), F32), pltpu.VMEM((16, 8, 128), F32),
        pltpu.VMEM((8, 128), F32), pltpu.VMEM((4, 8, 128), F32),
        pltpu.VMEM((16, 8, 128), F32), pltpu.VMEM((16, 8, 128), F32),
        pltpu.VMEM((4, 2, 256, 128), BF16), pltpu.VMEM((4, 8, 64, 128), BF16),
        pltpu.VMEM((2, 24, 128), F32), pltpu.VMEM((8, 24, 128), F32),
        pltpu.VMEM((16, 64, 256), F32),
        dma((8,)), dma((16,)), dma((4, 8)), dma((4, 8)), dma((4,)), dma((4,)), dma, dma,
        dma((16,)), dma((16,)), dma((4,)), dma((4,)), dma((16,)), dma((16,)),
        dma((4, 2, 4)), dma((4, 8)), dma((2, 4)), dma((8,)),
    ]
    return pl.pallas_call(
        kernel,
        out_shape=(
            jax.ShapeDtypeStruct((16, 64, 256), F32),
            jax.ShapeDtypeStruct((2, 4), F32),
            jax.ShapeDtypeStruct((2, 4), F32),
        ),
        in_specs=[anywhere] * 8,
        out_specs=(anywhere, vmem, vmem),
        scratch_shapes=scratch,
        compiler_params=pltpu.CompilerParams(collective_id=0, has_side_effects=True),
    )(forcing, starting_heat, half, rest, *tables)


def solution(mesh):
    torus = Mesh(mesh.devices.reshape(NX, NZ, 2, mesh.shape["space"]), (X, Z, CORE, Y))
    times = (X, Z, CORE)
    in_specs = (P(times, Y, None), P(Y, None))
    out_specs = (P(times, Y, None), P(None, times), P(None, times))
    return jax.shard_map(per_device, mesh=torus, in_specs=in_specs, out_specs=out_specs, check_vma=False)
```

```python
import math

import jax
import jax.numpy as jnp
import numpy as np
from jax import lax
from jax.experimental import pallas as pl
from jax.experimental.pallas import tpu as pltpu
from jax.sharding import Mesh
from jax.sharding import PartitionSpec as P

GRID = 256
NT = 2048
STEP = 0.004 / NT
X, Z, CORE, Y = "tm_0", "tm_1", "tm_2", "space"
NX, NZ = 4, 16
PHASES = 4
F32, BF16 = jnp.float32, jnp.bfloat16


def sine_tables():
    numbers = np.arange(1, GRID + 1)
    product = numbers[:, None] * numbers[None, :] % (2 * (GRID + 1))
    angles = (np.float32(np.pi) * product.astype(np.float32)) / np.float32(GRID + 1)
    table = (np.float32(math.sqrt(2.0 / (GRID + 1))) * np.sin(angles.astype(np.float64))).astype(np.float32)
    half = table.astype(jnp.bfloat16)
    rest = (table - half.astype(np.float32)).astype(jnp.bfloat16)
    return half, rest


def mode_tables():
    mu = (4.0 * (GRID + 1) ** 2 * np.sin(np.pi * np.arange(1, GRID + 1) / (2 * (GRID + 1))) ** 2).astype(np.float32)
    lane = np.arange(128)
    rows = np.broadcast_to(mu[:, None], (GRID, 128))
    packed = mu[64 * (lane // 32)[None, :] + np.arange(64)[:, None]]
    tiles = np.concatenate([packed.reshape(NZ, 4, 128)] * 2, axis=1)
    columns = np.broadcast_to(mu.reshape(8, 1, 32)[:, :, lane % 32], (8, 8, 128))
    return tuple(np.ascontiguousarray(t) for t in (rows, packed, tiles, columns))


def lane_group():
    return lax.broadcasted_iota(jnp.int32, (64, 128), 1) // 32


def turn(parts):
    group = lane_group()
    rolled = [parts[0]] + [pltpu.roll(parts[a], 32 * a, 1) for a in range(1, 4)]
    out = []
    for b in range(4):
        pick = [rolled[(g - b) % 4] for g in range(4)]
        mixed = jnp.where(
            group < 2, jnp.where(group == 0, pick[0], pick[1]), jnp.where(group == 2, pick[2], pick[3])
        )
        out.append(pltpu.roll(mixed, 128 - 32 * b, 1) if b else mixed)
    return out


def dot(a, b):
    return jnp.dot(a, b, preferred_element_type=F32)


class Weights:
    def __init__(self, x):
        one = 1.0
        gain = one / (one + x)
        y = 4.0 * x
        psi = one / (one + y)
        self.lift = lift = one + 16.0 * x
        theta = one / lift
        square = gain * gain
        phi = square * square
        psi2 = psi * psi
        psi3 = psi2 * psi
        psi4 = psi2 * psi2
        less = -(x * x * (6.0 + 4.0 * x + x * x)) * phi * psi
        deep = -(y * y * (6.0 + 4.0 * y + y * y)) * psi4 * theta
        big = phi * less
        alpha = 3.0 * big * psi2
        beta = psi3 * (big * psi3 + phi * deep)
        xb = psi3 * phi * lift
        c2 = psi4 * psi * big * phi - beta * xb
        c1 = 2.0 * big * phi * psi - alpha * xb
        kappa = (less * psi3 + deep) * lift
        bl2 = beta * lift * lift
        w1 = (phi * psi2, phi * psi, phi, xb)
        own = (psi4 * big * phi * lift, psi3 * big * phi * lift, None, (c1 + c2 * lift) * lift)
        w3 = tuple(bl2 * a if b is None else bl2 * a - b for a, b in zip(w1, own))
        self.w1 = w1
        self.w2 = (big * phi - w3[0], -w3[1], -w3[2], -w3[3])
        self.w3 = w3
        self.w4 = (less * phi * psi - kappa * w1[0], less * phi - kappa * w1[1], -kappa * w1[2], -kappa * w1[3])
        self.d2 = less * phi * psi2 - kappa * psi3 * phi
        self.e2 = -c2 * lift
        self.alpha = alpha + beta * lift
        self.gain, self.phi, self.psi, self.theta = gain, phi, psi, theta
        self.less, self.deep, self.xb, self.kappa = less, deep, xb, kappa


def weighted(weights, parts):
    total = weights[0] * parts[0]
    for w, part in zip(weights[1:], parts[1:]):
        total = total + w * part
    return total


def corrections(w, first, residual):
    out = []
    p, q = first, None
    for c in range(3):
        p = w.psi * p + residual[c]
        q = residual[c] if q is None else w.psi * q + residual[c]
        out.append(p)
    out.append(w.theta * first + (w.psi * q + residual[3]))
    return out


def kernel(
    forcing, starting, sine, sine_rest, mu_rows, mu_packed, mu_tiles, mu_columns,
    recv_o, recv_s,
    fin, sin, sh, sr, mrow, mpack, mtile, mcol,
    send_a, recv_a, send_u, recv_u, start_c, src, send_n, recv_n,
    send_z, recv_z, send_x, recv_x, send_b, recv_b, send_o, send_s,
    load_sem, own_sem, met, sa, ra, su, ru, sn, rn, sz, rz, sx, rx, sb, rb, so, ro, ss, rs,
):
    x, z, core, y = (lax.axis_index(a) for a in (X, Z, CORE, Y))
    me = 2 * y + core
    zn, zp = lax.rem(z + 1, NZ), lax.rem(z + NZ - 1, NZ)
    xn = jnp.where(z == NZ - 1, lax.rem(x + 1, NX), x)
    xp = jnp.where(z == 0, lax.rem(x + NX - 1, NX), x)
    my_rows = pl.ds(pl.multiple_of(64 * y, 64), 64)

    barrier = pltpu.get_barrier_semaphore()
    for k in range(1, 8):
        d = lax.rem(me + k, 8)
        pl.semaphore_signal(barrier, inc=1, device_id={Y: d // 2, CORE: lax.rem(d, 2)})
    pl.semaphore_signal(barrier, inc=1, device_id={Z: zn})
    pl.semaphore_signal(barrier, inc=1, device_id={Z: zp})
    for k in range(1, NX):
        pl.semaphore_signal(barrier, inc=1, device_id={X: lax.rem(x + k, NX)})
    pl.semaphore_signal(barrier, inc=1, device_id={X: xn, Z: zn})
    pl.semaphore_signal(barrier, inc=1, device_id={X: xp, Z: zp})

    loads = [
        (forcing, fin), (sine, sh), (sine_rest, sr), (starting, sin), (mu_rows, mrow), (mu_packed, mpack),
        (mu_tiles.at[z], mtile), (mu_columns.at[me], mcol),
    ]
    loads = [pltpu.make_async_copy(a, b, load_sem.at[i]) for i, (a, b) in enumerate(loads)]
    for copy in loads:
        copy.start()

    def greet(r):
        for k in (2**r, NZ - 2**r):
            pl.semaphore_signal(met.at[r], inc=1, device_id={Z: lax.rem(z + k, NZ)})

    loads[0].wait()
    loads[1].wait()
    table = sh[...]

    def halves(p):
        fields = jnp.concatenate([fin[4 * c + p] for c in range(4)], axis=0)
        product = dot(fields, table)
        for side in range(2):
            for q, part in enumerate(turn([product[64 * c : 64 * c + 64, 128 * side : 128 * side + 128] for c in range(4)])):
                send_a[p, 4 * side + q] = part.astype(BF16)

    def copy_a(p, d, source, from_core, rows):
        return pltpu.make_async_remote_copy(
            src_ref=send_a.at[p, d], dst_ref=recv_a.at[p, from_core, rows],
            send_sem=sa.at[p, d], recv_sem=ra.at[p, source], device_id={Y: d // 2, CORE: d % 2},
        )

    for p in range(PHASES):
        halves(p)
        if p == 0:
            pl.semaphore_wait(barrier, 14)
            greet(0)
        for d in range(8):
            @pl.when(d != me)
            def _():
                copy_a(p, d, me, core, my_rows).start()

            @pl.when(d == me)
            def _():
                recv_a[p, core, my_rows] = send_a[p, d]

    first = jnp.logical_and(x == 0, z == 0)
    loads[3].wait()

    def copy_u(k, source):
        return pltpu.make_async_remote_copy(
            src_ref=send_u.at[k], dst_ref=recv_u.at[pl.ds(pl.multiple_of(64 * source, 64), 64)],
            send_sem=su.at[k], recv_sem=ru.at[source], device_id={Y: k},
        )

    @pl.when(first)
    def _():
        product = dot(sin[...], table)
        for k in range(4):
            side = product[:, 128 * (k // 2) : 128 * (k // 2) + 128]
            shift = 2 * (k % 2)
            even = pltpu.roll(side, (128 - 32 * shift) % 128, 1) if shift else side
            odd = pltpu.roll(side, (128 - 32 * (shift + 1)) % 128, 1)
            send_u[k] = jnp.where(core == 0, even, odd).astype(BF16)
        for k in range(4):
            @pl.when(k != y)
            def _():
                copy_u(k, y).start()

            @pl.when(k == y)
            def _():
                recv_u[my_rows] = send_u[k]

    for i in (2, 4, 5, 6, 7):
        loads[i].wait()
    gain = 1.0 / (1.0 + STEP * (mrow[...] + mcol[0:1, :]))
    w = Weights(STEP * (mpack[...] + mcol[0:1, :]))
    wo = Weights(STEP * (mtile[...] + mcol[...]))
    lower = lax.broadcasted_iota(jnp.int32, (8, 128), 0) < 4
    hop = wo.theta * wo.theta
    cross = jnp.where(lower, 0.0, 2.0 * wo.theta * wo.alpha)
    powers = [(jnp.ones_like(hop), jnp.zeros_like(hop))]
    for k in range(NZ):
        t, c = powers[-1]
        powers.append((hop * t, hop * c + cross * t))

    pl.semaphore_wait(met.at[0], 2)
    greet(1)

    @pl.when(first)
    def _():
        for k in range(4):
            @pl.when(k != y)
            def _():
                copy_u(k, k).wait_recv()
        modes = dot(table, recv_u[...])
        group = lane_group()
        total = jnp.where(group == 0, modes[0:64], 0.0)
        for r in range(1, 4):
            total = jnp.where(group == r, pltpu.roll(modes[64 * r : 64 * r + 64], 32 * r, 1), total)
        start_c[...] = total

    @pl.when(jnp.logical_not(first))
    def _():
        start_c[...] = jnp.zeros_like(start_c)

    for p in range(PHASES):
        for s in range(8):
            @pl.when(s != me)
            def _():
                copy_a(p, s, s, s % 2, pl.ds(64 * (s // 2), 64)).wait_recv()
        if p == 0:
            pl.semaphore_wait(met.at[1], 2)
            greet(2)
        for h in range(2):
            src[p, h] = gain * dot(table, recv_a[p, h])

    points = []
    for h in range(2):
        s = gain * src[0, h] + src[1, h]
        s = gain * s + src[2, h]
        s = gain * s + src[3, h]
        points.append(turn([s[64 * r : 64 * r + 64] for r in range(4)]))
    start = start_c[...]
    points[0][0] = points[0][0] + w.phi * start

    f = [weighted(w.w1, points[h]) for h in range(2)]
    g = [weighted(w.w2, points[h]) for h in range(2)]
    f_all = w.theta * f[0] + f[1]
    g_all = w.theta * g[0] + w.alpha * f[0] + g[1]
    for v in range(8):
        a, b = f_all[8 * v : 8 * v + 8], g_all[8 * v : 8 * v + 8]
        send_z[2 * v] = jnp.where(lower, a, pltpu.roll(b, 4, 0))
        send_z[2 * v + 1] = jnp.where(lower, pltpu.roll(a, 4, 0), b)

    def copy_z(to, source):
        return pltpu.make_async_remote_copy(
            src_ref=send_z.at[to], dst_ref=recv_z.at[source],
            send_sem=sz.at[to], recv_sem=rz.at[source], device_id={Z: to},
        )

    pl.semaphore_wait(met.at[2], 2)
    far_first = sorted(range(1, NZ), key=lambda k: -min(k, NZ - k))
    for k in far_first:
        copy_z(lax.rem(z + k, NZ), z).start()
    recv_z[z] = send_z[z]

    send_n[0] = points[1][3]
    send_n[1] = weighted(w.w4, points[1]) + w.d2 * points[0][3]
    send_n[2] = weighted(w.w3, points[1]) + w.e2 * points[0][3]
    copy_n = pltpu.make_async_remote_copy(
        src_ref=send_n, dst_ref=recv_n, send_sem=sn, recv_sem=rn, device_id={X: xn, Z: zn}
    )
    copy_n.start()

    for k in far_first[::-1]:
        source = lax.rem(z + k, NZ)
        copy_z(source, source).wait_recv()
    plain, coupled = [jnp.zeros((8, 128), F32)], [jnp.zeros((8, 128), F32)]
    for k in range(NZ):
        plain.append(hop * plain[-1] + recv_z[k])
    for k in range(NZ):
        coupled.append(hop * coupled[-1] + cross * pltpu.roll(plain[k], 4, 0))
    states = [a + b for a, b in zip(plain, coupled)]
    send_x[...] = states[NZ]

    def copy_x(to, source, k):
        return pltpu.make_async_remote_copy(
            src_ref=send_x, dst_ref=recv_x.at[source], send_sem=sx.at[k], recv_sem=rx.at[source], device_id={X: to}
        )

    for k in range(1, NX):
        copy_x(lax.rem(x + k, NX), x, k).start()
    for k in range(1, NX):
        source = lax.rem(x + k, NX)
        copy_x(source, source, k).wait_recv()
    recv_x[x] = states[NZ]
    entering = jnp.zeros((8, 128), F32)
    for k in range(NX - 1):
        further = powers[NZ][0] * entering + powers[NZ][1] * pltpu.roll(entering, 4, 0) + recv_x[k]
        entering = jnp.where(k < x, further, entering)
    turned = pltpu.roll(entering, 4, 0)
    for k in range(NZ):
        send_b[k] = states[k] + (powers[k][0] * entering + powers[k][1] * turned)

    def copy_b(to, source):
        return pltpu.make_async_remote_copy(
            src_ref=send_b.at[to], dst_ref=recv_b.at[source],
            send_sem=sb.at[to], recv_sem=rb.at[source], device_id={Z: to},
        )

    for k in far_first:
        copy_b(lax.rem(z + k, NZ), z).start()
    recv_b[z] = send_b[z]

    copy_n.wait_recv()
    keep = jnp.logical_not(first)
    near = [jnp.where(keep, recv_n[i], 0.0) for i in range(3)]
    residual_a = [near[0], points[0][3]]
    near_d = [near[1], weighted(w.w4, points[0]) + w.d2 * near[0]]
    near_e = [near[2], weighted(w.w3, points[0]) + w.e2 * near[0]]

    for k in far_first[::-1]:
        source = lax.rem(z + k, NZ)
        copy_b(source, source).wait_recv()
    fs, gs = [], []
    for v in range(8):
        a, b = recv_b[2 * v], recv_b[2 * v + 1]
        fs.append(jnp.where(lower, a, pltpu.roll(b, 4, 0)))
        gs.append(jnp.where(lower, pltpu.roll(a, 4, 0), b))
    f_in = jnp.concatenate(fs, axis=0)
    g_in = jnp.concatenate(gs, axis=0)

    sums = []
    for h in range(2):
        if h == 1:
            g_in = w.theta * g_in + w.alpha * f_in + g[0]
            f_in = w.theta * f_in + f[0]
        s = points[h]
        a = residual_a[h]
        e1 = f_in - w.xb * a
        d = w.kappa * f_in + near_d[h]
        e2 = g_in + near_e[h]
        r1 = [w.phi * a] + [w.phi * s[c] for c in range(3)]
        p1 = corrections(w, e1, r1)
        later = [w.less * e1, w.less * p1[0], w.less * p1[1], w.less * p1[2] + w.deep * e1]
        r2 = [w.phi * d] + [w.phi * later[c] for c in range(3)]
        p2 = corrections(w, e2, r2)
        v1 = [s[c] + p1[c] for c in range(4)]
        v2 = [v1[c] + later[c] + p2[c] for c in range(4)]
        enter = a + e1 + d + e2
        if h == 0:
            enter = enter + start
        squares = [jnp.sum(q * q, axis=0, keepdims=True) for q in r1 + r2 + p1 + p2 + v1 + v2]
        sums.append(squares)
        begin = jnp.concatenate(turn([enter, v2[0], v2[1], v2[2]]), axis=0)
        ends = jnp.concatenate(turn(v2), axis=0)
        u = begin
        for p in range(3):
            u = gain * u + src[p, h]
            src[p, h] = u
        src[3, h] = ends

    def copy_o(p, h, k, source):
        return pltpu.make_async_remote_copy(
            src_ref=send_o.at[p, h, pl.ds(64 * k, 64)], dst_ref=recv_o.at[p, source],
            send_sem=so.at[p, h, k], recv_sem=ro.at[p, source], device_id={Y: k, CORE: h},
        )

    def keep_o(p, h, k):
        return pltpu.make_async_copy(send_o.at[p, h, pl.ds(64 * k, 64)], recv_o.at[p, me], own_sem.at[p])

    def keep_s(h):
        return pltpu.make_async_copy(send_s.at[h], recv_s.at[me], own_sem.at[4])

    rest = sr[...]
    for p in range(PHASES):
        for h in range(2):
            u = src[p, h]
            high = u.astype(BF16)
            low = (u - high.astype(F32)).astype(BF16)
            send_o[p, h] = (dot(table, high) + (dot(table, low) + dot(rest, high))).astype(BF16)
        for h in range(2):
            for k in range(4):
                @pl.when(2 * k + h != me)
                def _():
                    copy_o(p, h, k, me).start()

                @pl.when(2 * k + h == me)
                def _():
                    keep_o(p, h, k).start()

    def copy_s(h, k, source):
        return pltpu.make_async_remote_copy(
            src_ref=send_s.at[h], dst_ref=recv_s.at[source],
            send_sem=ss.at[h, k], recv_sem=rs.at[source], device_id={Y: k, CORE: h},
        )

    for h in range(2):
        send_s[h] = jnp.concatenate(sums[h], axis=0)
    for h in range(2):
        for k in range(4):
            @pl.when(2 * k + h != me)
            def _():
                copy_s(h, k, me).start()

            @pl.when(2 * k + h == me)
            def _():
                keep_s(h).start()

    for p in range(PHASES):
        for s in range(8):
            @pl.when(s != me)
            def _():
                copy_o(p, s % 2, s // 2, s).wait_recv()
    for s in range(8):
        @pl.when(s != me)
        def _():
            copy_s(s % 2, s // 2, s).wait_recv()
    for p in range(PHASES):
        for d in range(8):
            @pl.when(d != me)
            def _():
                copy_a(p, d, me, core, my_rows).wait_send()
                copy_o(p, d % 2, d // 2, me).wait_send()

            @pl.when(d == me)
            def _():
                keep_o(p, d % 2, d // 2).wait()

    for d in range(8):
        @pl.when(d != me)
        def _():
            copy_s(d % 2, d // 2, me).wait_send()

        @pl.when(d == me)
        def _():
            keep_s(d % 2).wait()

    @pl.when(first)
    def _():
        for k in range(4):
            @pl.when(k != y)
            def _():
                copy_u(k, y).wait_send()

    copy_n.wait_send()
    for k in range(1, NZ):
        to = lax.rem(z + k, NZ)
        copy_z(to, z).wait_send()
        copy_b(to, z).wait_send()
    for k in range(1, NX):
        copy_x(lax.rem(x + k, NX), x, k).wait_send()


def finish(rows, squares, sine, heat, history, change):
    sides = []
    for side in range(2):
        sides.append(turn([rows[0, 4 * side + q].astype(F32) for q in range(4)]))
    stacked = jnp.concatenate(
        [jnp.concatenate([sides[0][c], sides[1][c]], axis=1) for c in range(4)], axis=0
    ).astype(BF16)
    field = dot(stacked, sine[...])
    for c in range(4):
        heat[c, 0] = field[64 * c : 64 * c + 64]

    @pl.when(pl.program_id(0) == 0)
    def _():
        total = squares[0]
        for s in range(1, 8):
            total = total + squares[s]
        total = jnp.sum(total, axis=1, keepdims=True)
        norms = jnp.sqrt(total[0:8] / (GRID * GRID))
        ratios = jnp.sqrt(total[8:16] / total[16:24])
        mine = lax.broadcasted_iota(jnp.int32, (8, 128), 1) == lax.broadcasted_iota(jnp.int32, (8, 128), 0) % 4
        for column, out in ((norms, history), (ratios, change)):
            spread = jnp.where(mine, column, 0.0)
            for i in range(2):
                out[i : i + 1, :] = jnp.sum(spread[4 * i : 4 * i + 4], axis=0, keepdims=True)[:, 0:4]


def per_device(forcing, starting_heat):
    half, rest = sine_tables()
    tables = mode_tables()
    anywhere = pl.BlockSpec(memory_space=pl.ANY)
    dma = pltpu.SemaphoreType.DMA
    scratch = [
        pltpu.VMEM((16, 64, 256), BF16), pltpu.VMEM((64, 256), BF16),
        pltpu.VMEM((256, 256), BF16), pltpu.VMEM((256, 256), BF16),
        pltpu.VMEM((256, 128), F32), pltpu.VMEM((64, 128), F32),
        pltpu.VMEM((8, 128), F32), pltpu.VMEM((8, 128), F32),
        pltpu.VMEM((4, 8, 64, 128), BF16), pltpu.VMEM((4, 2, 256, 128), BF16),
        pltpu.VMEM((4, 64, 128), BF16), pltpu.VMEM((256, 128), BF16), pltpu.VMEM((64, 128), F32),
        pltpu.VMEM((4, 2, 256, 128), F32), pltpu.VMEM((3, 64, 128), F32), pltpu.VMEM((3, 64, 128), F32),
        pltpu.VMEM((16, 8, 128), F32), pltpu.VMEM((16, 8, 128), F32),
        pltpu.VMEM((8, 128), F32), pltpu.VMEM((4, 8, 128), F32),
        pltpu.VMEM((16, 8, 128), F32), pltpu.VMEM((16, 8, 128), F32),
        pltpu.VMEM((4, 2, 256, 128), BF16), pltpu.VMEM((2, 24, 128), F32),
        dma((8,)), dma((5,)), pltpu.SemaphoreType.REGULAR((3,)), dma((4, 8)), dma((4, 8)), dma((4,)), dma((4,)), dma, dma,
        dma((16,)), dma((16,)), dma((4,)), dma((4,)), dma((16,)), dma((16,)),
        dma((4, 2, 4)), dma((4, 8)), dma((2, 4)), dma((8,)),
    ]
    rows, squares = pl.pallas_call(
        kernel,
        out_shape=(jax.ShapeDtypeStruct((4, 8, 64, 128), BF16), jax.ShapeDtypeStruct((8, 24, 128), F32)),
        in_specs=[anywhere] * 8,
        out_specs=(anywhere, anywhere),
        scratch_shapes=scratch,
        compiler_params=pltpu.CompilerParams(collective_id=0, has_side_effects=True),
    )(forcing, starting_heat, half, rest, *tables)
    heat, history, change = pl.pallas_call(
        finish,
        grid=(PHASES,),
        out_shape=(
            jax.ShapeDtypeStruct((4, PHASES, 64, 256), F32),
            jax.ShapeDtypeStruct((2, 4), F32),
            jax.ShapeDtypeStruct((2, 4), F32),
        ),
        in_specs=[
            pl.BlockSpec((1, 8, 64, 128), lambda p: (p, 0, 0, 0)),
            pl.BlockSpec((8, 24, 128), lambda p: (0, 0, 0)),
            pl.BlockSpec((256, 256), lambda p: (0, 0)),
        ],
        out_specs=(
            pl.BlockSpec((4, 1, 64, 256), lambda p: (0, p, 0, 0)),
            pl.BlockSpec((2, 4), lambda p: (0, 0)),
            pl.BlockSpec((2, 4), lambda p: (0, 0)),
        ),
    )(rows, squares, half)
    return heat.reshape(forcing.shape), history, change


def solution(mesh):
    torus = Mesh(mesh.devices.reshape(NX, NZ, 2, mesh.shape["space"]), (X, Z, CORE, Y))
    times = (X, Z, CORE)
    in_specs = (P(times, Y, None), P(Y, None))
    out_specs = (P(times, Y, None), P(None, times), P(None, times))
    return jax.shard_map(per_device, mesh=torus, in_specs=in_specs, out_specs=out_specs, check_vma=False)
```

```python
import math

import jax
import jax.numpy as jnp
import numpy as np
from jax import lax
from jax.experimental import pallas as pl
from jax.experimental.pallas import tpu as pltpu
from jax.sharding import Mesh
from jax.sharding import PartitionSpec as P

GRID = 256
NT = 2048
STEP = 0.004 / NT
X, Z, CORE, Y = "tm_0", "tm_1", "tm_2", "space"
NX, NZ = 4, 16
PHASES = 4
F32, BF16 = jnp.float32, jnp.bfloat16


def sine_tables():
    numbers = np.arange(1, GRID + 1)
    product = numbers[:, None] * numbers[None, :] % (2 * (GRID + 1))
    angles = (np.float32(np.pi) * product.astype(np.float32)) / np.float32(GRID + 1)
    table = (np.float32(math.sqrt(2.0 / (GRID + 1))) * np.sin(angles.astype(np.float64))).astype(np.float32)
    half = table.astype(jnp.bfloat16)
    rest = (table - half.astype(np.float32)).astype(jnp.bfloat16)
    return half, rest


def mode_tables():
    mu = (4.0 * (GRID + 1) ** 2 * np.sin(np.pi * np.arange(1, GRID + 1) / (2 * (GRID + 1))) ** 2).astype(np.float32)
    lane = np.arange(128)
    rows = np.broadcast_to(mu[:, None], (GRID, 128))
    packed = mu[64 * (lane // 32)[None, :] + np.arange(64)[:, None]]
    tiles = np.concatenate([packed.reshape(NZ, 4, 128)] * 2, axis=1)
    columns = np.broadcast_to(mu.reshape(8, 1, 32)[:, :, lane % 32], (8, 8, 128))
    return tuple(np.ascontiguousarray(t) for t in (rows, packed, tiles, columns))


def lane_group():
    return lax.broadcasted_iota(jnp.int32, (64, 128), 1) // 32


def turn(parts):
    group = lane_group()
    rolled = [parts[0]] + [pltpu.roll(parts[a], 32 * a, 1) for a in range(1, 4)]
    out = []
    for b in range(4):
        pick = [rolled[(g - b) % 4] for g in range(4)]
        mixed = jnp.where(
            group < 2, jnp.where(group == 0, pick[0], pick[1]), jnp.where(group == 2, pick[2], pick[3])
        )
        out.append(pltpu.roll(mixed, 128 - 32 * b, 1) if b else mixed)
    return out


def dot(a, b):
    return jnp.dot(a, b, preferred_element_type=F32)


def taken(sem, ref):
    pltpu.make_async_copy(ref, ref, sem).wait()


class Weights:
    def __init__(self, x):
        one = 1.0
        gain = one / (one + x)
        y = 4.0 * x
        psi = one / (one + y)
        self.lift = lift = one + 16.0 * x
        theta = one / lift
        square = gain * gain
        phi = square * square
        psi2 = psi * psi
        psi3 = psi2 * psi
        psi4 = psi2 * psi2
        less = -(x * x * (6.0 + 4.0 * x + x * x)) * phi * psi
        deep = -(y * y * (6.0 + 4.0 * y + y * y)) * psi4 * theta
        big = phi * less
        alpha = 3.0 * big * psi2
        beta = psi3 * (big * psi3 + phi * deep)
        xb = psi3 * phi * lift
        c2 = psi4 * psi * big * phi - beta * xb
        c1 = 2.0 * big * phi * psi - alpha * xb
        kappa = (less * psi3 + deep) * lift
        bl2 = beta * lift * lift
        w1 = (phi * psi2, phi * psi, phi, xb)
        own = (psi4 * big * phi * lift, psi3 * big * phi * lift, None, (c1 + c2 * lift) * lift)
        w3 = tuple(bl2 * a if b is None else bl2 * a - b for a, b in zip(w1, own))
        self.w1 = w1
        self.w2 = (big * phi - w3[0], -w3[1], -w3[2], -w3[3])
        self.w3 = w3
        self.w4 = (less * phi * psi - kappa * w1[0], less * phi - kappa * w1[1], -kappa * w1[2], -kappa * w1[3])
        self.d2 = less * phi * psi2 - kappa * psi3 * phi
        self.e2 = -c2 * lift
        self.alpha = alpha + beta * lift
        self.gain, self.phi, self.psi, self.theta = gain, phi, psi, theta
        self.less, self.deep, self.xb, self.kappa = less, deep, xb, kappa


def weighted(weights, parts):
    total = weights[0] * parts[0]
    for w, part in zip(weights[1:], parts[1:]):
        total = total + w * part
    return total


def corrections(w, first, residual):
    out = []
    p, q = first, None
    for c in range(3):
        p = w.psi * p + residual[c]
        q = residual[c] if q is None else w.psi * q + residual[c]
        out.append(p)
    out.append(w.theta * first + (w.psi * q + residual[3]))
    return out


def kernel(
    forcing, starting, sine, sine_rest, mu_rows, mu_packed, mu_tiles, mu_columns,
    hout, history, change,
    fin, sin, sh, sr, mrow, mpack, mtile, mcol,
    send_a, recv_a, send_u, recv_u, start_c, src, send_n, recv_n,
    send_z, recv_z, send_x, recv_x, send_b, recv_b, send_o, recv_o, send_s, recv_s,
    load_sem, met, sa, ra, su, ru, sn, rn, sz, rz, sx, rx, sb, rb, so, ro, ss, rs,
):
    x, z, core, y = (lax.axis_index(a) for a in (X, Z, CORE, Y))
    me = 2 * y + core
    zn, zp = lax.rem(z + 1, NZ), lax.rem(z + NZ - 1, NZ)
    xn = jnp.where(z == NZ - 1, lax.rem(x + 1, NX), x)
    xp = jnp.where(z == 0, lax.rem(x + NX - 1, NX), x)
    my_rows = pl.ds(pl.multiple_of(64 * y, 64), 64)

    barrier = pltpu.get_barrier_semaphore()
    for k in range(1, 8):
        d = lax.rem(me + k, 8)
        pl.semaphore_signal(barrier, inc=1, device_id={Y: d // 2, CORE: lax.rem(d, 2)})
    pl.semaphore_signal(barrier, inc=1, device_id={Z: zn})
    pl.semaphore_signal(barrier, inc=1, device_id={Z: zp})
    for k in range(1, NX):
        pl.semaphore_signal(barrier, inc=1, device_id={X: lax.rem(x + k, NX)})
    pl.semaphore_signal(barrier, inc=1, device_id={X: xn, Z: zn})
    pl.semaphore_signal(barrier, inc=1, device_id={X: xp, Z: zp})

    loads = [
        (sine, sh), (sine_rest, sr), (starting, sin), (mu_rows, mrow), (mu_packed, mpack), (mu_tiles.at[z], mtile),
        (mu_columns.at[me], mcol),
    ]
    loads = [pltpu.make_async_copy(a, b, load_sem.at[i]) for i, (a, b) in enumerate(loads)]
    loads[0].start()
    for p in range(PHASES):
        for c in range(4):
            pltpu.make_async_copy(forcing.at[4 * c + p], fin.at[p, c], load_sem.at[7 + p]).start()

    def greet(r):
        for k in (2**r, NZ - 2**r):
            pl.semaphore_signal(met.at[r], inc=1, device_id={Z: lax.rem(z + k, NZ)})

    loads[0].wait()
    table = sh[...]

    def halves(p):
        product = dot(fin[p].reshape(256, 256), table)
        for side in range(2):
            for q, part in enumerate(turn([product[64 * c : 64 * c + 64, 128 * side : 128 * side + 128] for c in range(4)])):
                send_a[p, 4 * side + q] = part.astype(BF16)

    def copy_a(p, d):
        return pltpu.make_async_remote_copy(
            src_ref=send_a.at[p, d], dst_ref=recv_a.at[p, core, my_rows],
            send_sem=sa, recv_sem=ra.at[p], device_id={Y: d // 2, CORE: d % 2},
        )

    for p in range(PHASES):
        taken(load_sem.at[7 + p], fin.at[p])
        if p == 0:
            for copy in loads[1:]:
                copy.start()
        halves(p)
        if p == 0:
            pl.semaphore_wait(barrier, 14)
            greet(0)
        for d in range(8):
            @pl.when(d != me)
            def _():
                copy_a(p, d).start()

            @pl.when(d == me)
            def _():
                recv_a[p, core, my_rows] = send_a[p, d]

    first = jnp.logical_and(x == 0, z == 0)
    loads[2].wait()

    def copy_u(k):
        return pltpu.make_async_remote_copy(
            src_ref=send_u.at[k], dst_ref=recv_u.at[my_rows],
            send_sem=su, recv_sem=ru, device_id={Y: k},
        )

    @pl.when(first)
    def _():
        product = dot(sin[...], table)
        for k in range(4):
            side = product[:, 128 * (k // 2) : 128 * (k // 2) + 128]
            shift = 2 * (k % 2)
            even = pltpu.roll(side, (128 - 32 * shift) % 128, 1) if shift else side
            odd = pltpu.roll(side, (128 - 32 * (shift + 1)) % 128, 1)
            send_u[k] = jnp.where(core == 0, even, odd).astype(BF16)
        for k in range(4):
            @pl.when(k != y)
            def _():
                copy_u(k).start()

            @pl.when(k == y)
            def _():
                recv_u[my_rows] = send_u[k]

    for i in (1, 3, 4, 5, 6):
        loads[i].wait()
    gain = 1.0 / (1.0 + STEP * (mrow[...] + mcol[0:1, :]))
    w = Weights(STEP * (mpack[...] + mcol[0:1, :]))
    wo = Weights(STEP * (mtile[...] + mcol[...]))
    lower = lax.broadcasted_iota(jnp.int32, (8, 128), 0) < 4
    hop = wo.theta * wo.theta
    cross = jnp.where(lower, 0.0, 2.0 * wo.theta * wo.alpha)
    powers = [(jnp.ones_like(hop), jnp.zeros_like(hop))]
    for k in range(NZ):
        t, c = powers[-1]
        powers.append((hop * t, hop * c + cross * t))

    pl.semaphore_wait(met.at[0], 2)
    greet(1)

    @pl.when(first)
    def _():
        taken(ru, send_u.at[pl.ds(0, 3)])
        modes = dot(table, recv_u[...])
        group = lane_group()
        total = jnp.where(group == 0, modes[0:64], 0.0)
        for r in range(1, 4):
            total = jnp.where(group == r, pltpu.roll(modes[64 * r : 64 * r + 64], 32 * r, 1), total)
        start_c[...] = total

    @pl.when(jnp.logical_not(first))
    def _():
        start_c[...] = jnp.zeros_like(start_c)

    for p in range(PHASES):
        taken(ra.at[p], send_a.at[p, pl.ds(0, 7)])
        if p == 0:
            pl.semaphore_wait(met.at[1], 2)
            greet(2)
        for h in range(2):
            src[p, h] = gain * dot(table, recv_a[p, h])

    points = []
    for h in range(2):
        s = gain * src[0, h] + src[1, h]
        s = gain * s + src[2, h]
        s = gain * s + src[3, h]
        points.append(turn([s[64 * r : 64 * r + 64] for r in range(4)]))
    start = start_c[...]
    points[0][0] = points[0][0] + w.phi * start

    f = [weighted(w.w1, points[h]) for h in range(2)]
    g = [weighted(w.w2, points[h]) for h in range(2)]
    f_all = w.theta * f[0] + f[1]
    g_all = w.theta * g[0] + w.alpha * f[0] + g[1]
    for v in range(8):
        a, b = f_all[8 * v : 8 * v + 8], g_all[8 * v : 8 * v + 8]
        send_z[2 * v] = jnp.where(lower, a, pltpu.roll(b, 4, 0))
        send_z[2 * v + 1] = jnp.where(lower, pltpu.roll(a, 4, 0), b)

    def copy_z(to):
        return pltpu.make_async_remote_copy(
            src_ref=send_z.at[to], dst_ref=recv_z.at[z],
            send_sem=sz, recv_sem=rz, device_id={Z: to},
        )

    pl.semaphore_wait(met.at[2], 2)
    far_first = sorted(range(1, NZ), key=lambda k: -min(k, NZ - k))
    for k in far_first:
        copy_z(lax.rem(z + k, NZ)).start()
    recv_z[z] = send_z[z]

    send_n[0] = points[1][3]
    send_n[1] = weighted(w.w4, points[1]) + w.d2 * points[0][3]
    send_n[2] = weighted(w.w3, points[1]) + w.e2 * points[0][3]
    copy_n = pltpu.make_async_remote_copy(
        src_ref=send_n, dst_ref=recv_n, send_sem=sn, recv_sem=rn, device_id={X: xn, Z: zn}
    )
    copy_n.start()

    taken(rz, send_z.at[pl.ds(0, NZ - 1)])
    plain, coupled = [jnp.zeros((8, 128), F32)], [jnp.zeros((8, 128), F32)]
    for k in range(NZ):
        plain.append(hop * plain[-1] + recv_z[k])
    for k in range(NZ):
        coupled.append(hop * coupled[-1] + cross * pltpu.roll(plain[k], 4, 0))
    states = [a + b for a, b in zip(plain, coupled)]
    send_x[...] = states[NZ]

    def copy_x(to):
        return pltpu.make_async_remote_copy(
            src_ref=send_x, dst_ref=recv_x.at[x], send_sem=sx, recv_sem=rx, device_id={X: to}
        )

    for k in range(1, NX):
        copy_x(lax.rem(x + k, NX)).start()
    taken(rx, recv_x.at[pl.ds(0, NX - 1)])
    recv_x[x] = states[NZ]
    entering = jnp.zeros((8, 128), F32)
    for k in range(NX - 1):
        further = powers[NZ][0] * entering + powers[NZ][1] * pltpu.roll(entering, 4, 0) + recv_x[k]
        entering = jnp.where(k < x, further, entering)
    turned = pltpu.roll(entering, 4, 0)
    for k in range(NZ):
        send_b[k] = states[k] + (powers[k][0] * entering + powers[k][1] * turned)

    def copy_b(to):
        return pltpu.make_async_remote_copy(
            src_ref=send_b.at[to], dst_ref=recv_b.at[z],
            send_sem=sb, recv_sem=rb, device_id={Z: to},
        )

    for k in far_first:
        copy_b(lax.rem(z + k, NZ)).start()
    recv_b[z] = send_b[z]

    copy_n.wait_recv()
    keep = jnp.logical_not(first)
    near = [jnp.where(keep, recv_n[i], 0.0) for i in range(3)]
    residual_a = [near[0], points[0][3]]
    near_d = [near[1], weighted(w.w4, points[0]) + w.d2 * near[0]]
    near_e = [near[2], weighted(w.w3, points[0]) + w.e2 * near[0]]

    taken(rb, send_b.at[pl.ds(0, NZ - 1)])
    fs, gs = [], []
    for v in range(8):
        a, b = recv_b[2 * v], recv_b[2 * v + 1]
        fs.append(jnp.where(lower, a, pltpu.roll(b, 4, 0)))
        gs.append(jnp.where(lower, pltpu.roll(a, 4, 0), b))
    f_in = jnp.concatenate(fs, axis=0)
    g_in = jnp.concatenate(gs, axis=0)

    sums = []
    for h in range(2):
        if h == 1:
            g_in = w.theta * g_in + w.alpha * f_in + g[0]
            f_in = w.theta * f_in + f[0]
        s = points[h]
        a = residual_a[h]
        e1 = f_in - w.xb * a
        d = w.kappa * f_in + near_d[h]
        e2 = g_in + near_e[h]
        r1 = [w.phi * a] + [w.phi * s[c] for c in range(3)]
        p1 = corrections(w, e1, r1)
        later = [w.less * e1, w.less * p1[0], w.less * p1[1], w.less * p1[2] + w.deep * e1]
        r2 = [w.phi * d] + [w.phi * later[c] for c in range(3)]
        p2 = corrections(w, e2, r2)
        v1 = [s[c] + p1[c] for c in range(4)]
        v2 = [v1[c] + later[c] + p2[c] for c in range(4)]
        enter = a + e1 + d + e2
        if h == 0:
            enter = enter + start
        sums.append(r1 + r2 + p1 + p2 + v1 + v2)
        begin = jnp.concatenate(turn([enter, v2[0], v2[1], v2[2]]), axis=0)
        ends = jnp.concatenate(turn(v2), axis=0)
        u = begin
        for p in range(3):
            u = gain * u + src[p, h]
            src[p, h] = u
        src[3, h] = ends

    def copy_o(p, h, k):
        return pltpu.make_async_remote_copy(
            src_ref=send_o.at[p, h, pl.ds(64 * k, 64)], dst_ref=recv_o.at[p, me],
            send_sem=so, recv_sem=ro.at[p], device_id={Y: k, CORE: h},
        )

    def copy_s(h, k):
        return pltpu.make_async_remote_copy(
            src_ref=send_s.at[h], dst_ref=recv_s.at[me], send_sem=ss, recv_sem=rs, device_id={Y: k, CORE: h}
        )

    rest = sr[...]
    for p in range(PHASES):
        for h in range(2):
            u = src[p, h]
            high = u.astype(BF16)
            low = (u - high.astype(F32)).astype(BF16)
            send_o[p, h] = (dot(table, high) + (dot(table, low) + dot(rest, high))).astype(BF16)
        for h in range(2):
            for k in range(4):
                @pl.when(2 * k + h != me)
                def _():
                    copy_o(p, h, k).start()

                @pl.when(2 * k + h == me)
                def _():
                    recv_o[p, me] = send_o[p, h, 64 * k : 64 * k + 64]
        if p == 1:
            for h in range(2):
                send_s[h] = jnp.concatenate([jnp.sum(q * q, axis=0, keepdims=True) for q in sums[h]], axis=0)
            for h in range(2):
                for k in range(4):
                    @pl.when(2 * k + h != me)
                    def _():
                        copy_s(h, k).start()

                    @pl.when(2 * k + h == me)
                    def _():
                        recv_s[me] = send_s[h]
    for p in range(PHASES):
        if p == 3:
            taken(rs, recv_s.at[pl.ds(0, 7)])
            total = recv_s[0]
            for s in range(1, 8):
                total = total + recv_s[s]
            total = jnp.sum(total, axis=1, keepdims=True)
            norms = jnp.sqrt(total[0:8] / (GRID * GRID))
            ratios = jnp.sqrt(total[8:16] / total[16:24])
            mine = lax.broadcasted_iota(jnp.int32, (8, 128), 1) == lax.broadcasted_iota(jnp.int32, (8, 128), 0) % 4
            for column, result in ((norms, history), (ratios, change)):
                spread = jnp.where(mine, column, 0.0)
                for i in range(2):
                    result[i : i + 1, :] = jnp.sum(spread[4 * i : 4 * i + 4], axis=0, keepdims=True)[:, 0:4]
        taken(ro.at[p], send_a.at[p, pl.ds(0, 7)])
        sides = [turn([recv_o[p, 4 * side + q].astype(F32) for q in range(4)]) for side in range(2)]
        stacked = jnp.concatenate(
            [jnp.concatenate([sides[0][c], sides[1][c]], axis=1) for c in range(4)], axis=0
        ).astype(BF16)
        field = dot(stacked, table)
        for c in range(4):
            hout[4 * c + p] = field[64 * c : 64 * c + 64]

    taken(sa, send_a.at[:, pl.ds(0, 7)])
    taken(so, send_a.at[:, pl.ds(0, 7)])
    taken(ss, recv_s.at[pl.ds(0, 7)])

    @pl.when(first)
    def _():
        taken(su, send_u.at[pl.ds(0, 3)])

    copy_n.wait_send()
    taken(sz, send_z.at[pl.ds(0, NZ - 1)])
    taken(sb, send_b.at[pl.ds(0, NZ - 1)])
    taken(sx, recv_x.at[pl.ds(0, NX - 1)])


def put_out(a, b, c, heat, history, change, sem):
    copies = [pltpu.make_async_copy(s, d, sem.at[i]) for i, (s, d) in enumerate(((a, heat), (b, history), (c, change)))]
    for copy in copies:
        copy.start()
    for copy in copies:
        copy.wait()


def per_device(forcing, starting_heat):
    half, rest = sine_tables()
    tables = mode_tables()
    anywhere = pl.BlockSpec(memory_space=pl.ANY)
    vmem = pl.BlockSpec(memory_space=pltpu.VMEM)
    dma = pltpu.SemaphoreType.DMA
    scratch = [
        pltpu.VMEM((4, 4, 64, 256), BF16), pltpu.VMEM((64, 256), BF16),
        pltpu.VMEM((256, 256), BF16), pltpu.VMEM((256, 256), BF16),
        pltpu.VMEM((256, 128), F32), pltpu.VMEM((64, 128), F32),
        pltpu.VMEM((8, 128), F32), pltpu.VMEM((8, 128), F32),
        pltpu.VMEM((4, 8, 64, 128), BF16), pltpu.VMEM((4, 2, 256, 128), BF16),
        pltpu.VMEM((4, 64, 128), BF16), pltpu.VMEM((256, 128), BF16), pltpu.VMEM((64, 128), F32),
        pltpu.VMEM((4, 2, 256, 128), F32), pltpu.VMEM((3, 64, 128), F32), pltpu.VMEM((3, 64, 128), F32),
        pltpu.VMEM((16, 8, 128), F32), pltpu.VMEM((16, 8, 128), F32),
        pltpu.VMEM((8, 128), F32), pltpu.VMEM((4, 8, 128), F32),
        pltpu.VMEM((16, 8, 128), F32), pltpu.VMEM((16, 8, 128), F32),
        pltpu.VMEM((4, 2, 256, 128), BF16), pltpu.VMEM((4, 8, 64, 128), BF16),
        pltpu.VMEM((2, 24, 128), F32), pltpu.VMEM((8, 24, 128), F32),
        dma((11,)), pltpu.SemaphoreType.REGULAR((3,)), dma, dma((4,)), dma, dma, dma, dma,
        dma, dma, dma, dma, dma, dma, dma, dma((4,)), dma, dma,
    ]
    shapes = (forcing.shape, (2, 4), (2, 4))
    results = pl.pallas_call(
        kernel,
        out_shape=tuple(pltpu.VMEM(shape, F32) for shape in shapes),
        in_specs=[anywhere] * 8,
        out_specs=(vmem,) * 3,
        scratch_shapes=scratch,
        compiler_params=pltpu.CompilerParams(collective_id=0, has_side_effects=True),
    )(forcing, starting_heat, half, rest, *tables)
    results = [pltpu.with_memory_space_constraint(a, pltpu.VMEM) for a in results]
    return pl.pallas_call(
        put_out,
        out_shape=tuple(jax.ShapeDtypeStruct(shape, F32) for shape in shapes),
        in_specs=[vmem] * 3,
        out_specs=(anywhere,) * 3,
        scratch_shapes=[dma((3,))],
    )(*results)


def solution(mesh):
    torus = Mesh(mesh.devices.reshape(NX, NZ, 2, mesh.shape["space"]), (X, Z, CORE, Y))
    times = (X, Z, CORE)
    in_specs = (P(times, Y, None), P(Y, None))
    out_specs = (P(times, Y, None), P(None, times), P(None, times))
    return jax.shard_map(per_device, mesh=torus, in_specs=in_specs, out_specs=out_specs, check_vma=False)
```
